16 devices in a mesh: rep: 4 (over y, z, core), dp: 4 (over x).
Axes of the slice: x: 4, y: 2, z: 1, core: 2. Of those that a mesh axis runs over, the one named last changes fastest.
The devices are a block of a 4x4x8 slice.
Arguments:
- x: bfloat16 [16, 2048, 512], P(('rep', 'dp')), parts along dimension 0
- dy: bfloat16 [16, 2048, 512], P(('rep', 'dp')), parts along dimension 0
- wq: bfloat16 [2, 512, 768], replicated
- wk: bfloat16 [2, 512, 128], replicated
- wv: bfloat16 [2, 512, 128], replicated
- wo: bfloat16 [2, 768, 512], replicated
- w_gate: bfloat16 [2, 512, 2048], replicated
- w_up: bfloat16 [2, 512, 2048], replicated
- w_down: bfloat16 [2, 2048, 512], replicated
- m_wq: float32 [2, 512, 768], P(None, 'dp')
- m_wk: float32 [2, 512, 128], P(None, 'dp')
- m_wv: float32 [2, 512, 128], P(None, 'dp')
- m_wo: float32 [2, 768, 512], P(None, 'dp')
- m_w_gate: float32 [2, 512, 2048], P(None, 'dp')
- m_w_up: float32 [2, 512, 2048], P(None, 'dp')
- m_w_down: float32 [2, 2048, 512], P(None, 'dp')
- v_wq: float32 [2, 512, 768], P(None, 'dp')
- v_wk: float32 [2, 512, 128], P(None, 'dp')
- v_wv: float32 [2, 512, 128], P(None, 'dp')
- v_wo: float32 [2, 768, 512], P(None, 'dp')
- v_w_gate: float32 [2, 512, 2048], P(None, 'dp')
- v_w_up: float32 [2, 512, 2048], P(None, 'dp')
- v_w_down: float32 [2, 2048, 512], P(None, 'dp')
Outputs:
- output 1: bfloat16 [8, 512, 768], P('rep'), parts along dimension 0
- output 2: bfloat16 [8, 512, 128], P('rep'), parts along dimension 0
- output 3: bfloat16 [8, 512, 128], P('rep'), parts along dimension 0
- output 4: bfloat16 [8, 768, 512], P('rep'), parts along dimension 0
- output 5: bfloat16 [8, 512, 2048], P('rep'), parts along dimension 0
- output 6: bfloat16 [8, 512, 2048], P('rep'), parts along dimension 0
- output 7: bfloat16 [8, 2048, 512], P('rep'), parts along dimension 0
- output 8: float32 [8, 512, 768], P('rep', 'dp'), parts along dimension 0
- output 9: float32 [8, 512, 128], P('rep', 'dp'), parts along dimension 0
- output 10: float32 [8, 512, 128], P('rep', 'dp'), parts along dimension 0
- output 11: float32 [8, 768, 512], P('rep', 'dp'), parts along dimension 0
- output 12: float32 [8, 512, 2048], P('rep', 'dp'), parts along dimension 0
- output 13: float32 [8, 512, 2048], P('rep', 'dp'), parts along dimension 0
- output 14: float32 [8, 2048, 512], P('rep', 'dp'), parts along dimension 0
- output 15: float32 [8, 512, 768], P('rep', 'dp'), parts along dimension 0
- output 16: float32 [8, 512, 128], P('rep', 'dp'), parts along dimension 0
- output 17: float32 [8, 512, 128], P('rep', 'dp'), parts along dimension 0
- output 18: float32 [8, 768, 512], P('rep', 'dp'), parts along dimension 0
- output 19: float32 [8, 512, 2048], P('rep', 'dp'), parts along dimension 0
- output 20: float32 [8, 512, 2048], P('rep', 'dp'), parts along dimension 0
- output 21: float32 [8, 2048, 512], P('rep', 'dp'), parts along dimension 0
There are 4 independent parts. The reference program is written for one: setup_inputs(seed, part) draws one part's arguments, and reference() takes and returns one part's arrays. A program takes and returns all parts, laid end to end along the dimension named above; an argument that names none is the same for every part.
All inputs are finite; a program needn't handle non-finite values.
Results may differ from the reference program's by a relative error of at most 0.024.
Values are sent between devices in bfloat16 or wider.
A program may use at most 768 MiB of HBM per device.

```python
import jax
import jax.numpy as jnp
from jax import lax

SEQUENCES = 4
TOKENS = 2048
D = 512
HEADS = 6
KV_HEADS = 1
HEAD = 128
FF = 2048
LAYERS = 2
THETA = 10000
NAMES = ("wq", "wk", "wv", "wo", "w_gate", "w_up", "w_down")
SHAPES = {
    "wq": (LAYERS, D, HEADS * HEAD),
    "wk": (LAYERS, D, KV_HEADS * HEAD),
    "wv": (LAYERS, D, KV_HEADS * HEAD),
    "wo": (LAYERS, HEADS * HEAD, D),
    "w_gate": (LAYERS, D, FF),
    "w_up": (LAYERS, D, FF),
    "w_down": (LAYERS, FF, D),
}


def bump(key, n, height):
    away = (jnp.arange(n, dtype=jnp.int32) - jax.random.randint(key, (), 0, n, jnp.int32)) % n
    return jnp.where(away < n // 8, height, 1.0)


def together(key, own, strength):
    shared = jax.random.normal(key, own.shape[1:], jnp.float32)
    return (own + strength * shared) * lax.rsqrt(1 + strength * strength)


def setup_inputs(seed: int = 0, part: int = 0) -> dict:
    kx, kdy, ka, kb, kz, kf, kh, kl, *keys = jax.random.split(jax.random.key(seed), 8 + 3 * len(NAMES))
    kx, kdy, ka, kb = (jax.random.fold_in(k, part) for k in (kx, kdy, ka, kb))
    kw, km, kv = (keys[i::3] for i in range(3))
    shape = (SEQUENCES, TOKENS, D)
    much_x, much_dy = jax.random.uniform(kz, (2,), jnp.float32, 0.0, 1.0)
    loud = 2.0 ** jax.random.uniform(jax.random.fold_in(kz, 1), (), jnp.float32, -1.0, 2.0)
    layers = 2.0 ** jax.random.uniform(kl, (LAYERS, 1, 1), jnp.float32, -1.0, 1.0)
    times = {"wq": 1.0, "wk": 1.0, "wv": 2.0, "wo": layers, "w_gate": 1.0, "w_up": bump(kh, FF, 4.0), "w_down": layers}
    x = together(ka, jax.random.normal(kx, shape, jnp.float32), much_x) * bump(kf, D, 4.0)
    dy = together(kb, jax.random.normal(kdy, shape, jnp.float32), much_dy)
    drawn = {"x": x.astype(jnp.bfloat16), "dy": (loud * dy * (SEQUENCES * TOKENS) ** -0.5).astype(jnp.bfloat16)}
    for key, name in zip(kw, NAMES, strict=True):
        drawn[name] = (jax.random.normal(key, SHAPES[name], jnp.float32) * SHAPES[name][1] ** -0.5 * times[name]).astype(jnp.bfloat16)
    for key, name in zip(km, NAMES, strict=True):
        drawn[f"m_{name}"] = 0.1 * jax.random.normal(key, SHAPES[name], jnp.float32)
    for key, name in zip(kv, NAMES, strict=True):
        drawn[f"v_{name}"] = jax.random.uniform(key, SHAPES[name], jnp.float32, 0.02, 0.06)
    return drawn


def matmul(a, w):
    return jnp.dot(a, w, preferred_element_type=jnp.float32).astype(jnp.bfloat16)


def normed(h):
    wide = h.astype(jnp.float32)
    scale = lax.rsqrt(jnp.mean(wide**2, -1, keepdims=True) + 1e-6)
    return (wide * scale).astype(jnp.bfloat16)


def turned(t, theta):
    half = t.shape[-1] // 2
    angle = jnp.arange(t.shape[0], dtype=jnp.float32)[:, None] * theta ** (-jnp.arange(half, dtype=jnp.float32) / half)
    cos, sin = jnp.cos(angle)[:, None], jnp.sin(angle)[:, None]
    a, b = t[..., :half].astype(jnp.float32), t[..., half:].astype(jnp.float32)
    return jnp.concatenate([a * cos - b * sin, b * cos + a * sin], -1).astype(jnp.bfloat16)


def seen_by(q, k, v):
    tokens, kv = q.shape[0], k.shape[1]
    q = q.reshape(tokens, kv, -1, q.shape[-1])
    scores = jnp.einsum("tgsd,ugd->gstu", q.astype(jnp.float32), k.astype(jnp.float32)) * q.shape[-1] ** -0.5
    place = jnp.arange(tokens)
    weights = jax.nn.softmax(jnp.where(place[:, None] >= place, scores, -jnp.inf), -1).astype(jnp.bfloat16)
    return jnp.einsum("gstu,ugd->tgsd", weights.astype(jnp.float32), v.astype(jnp.float32)).astype(jnp.bfloat16).reshape(tokens, -1)


def layer(h, w):
    a = normed(h)
    q, k = (turned(matmul(a, w[name]).reshape(h.shape[0], -1, HEAD), THETA) for name in ("wq", "wk"))
    h = h + matmul(seen_by(q, k, matmul(a, w["wv"]).reshape(h.shape[0], -1, HEAD)), w["wo"])
    b = normed(h)
    gate = jnp.dot(b, w["w_gate"], preferred_element_type=jnp.float32)
    up = jnp.dot(b, w["w_up"], preferred_element_type=jnp.float32)
    return h + matmul((jax.nn.silu(gate) * up).astype(jnp.bfloat16), w["w_down"])


def adamw(w, m, v, g):
    m = 0.9 * m + 0.1 * g
    v = 0.95 * v + 0.05 * g * g
    step = m * lax.rsqrt(v + 1e-8) + 0.1 * w
    return (w - 0.02 * step).astype(jnp.bfloat16), m, v


def clipped(gradients, sum_of_squares, count):
    factor = jnp.minimum(1.0, 0.5 * lax.rsqrt(sum_of_squares / count + 1e-30))
    return [g * factor for g in gradients]


def stack(weights, h):
    return lax.scan(lambda h, w: (layer(h, w), None), h, weights)[0]


def reference(x, dy, wq, wk, wv, wo, w_gate, w_up, w_down, m_wq, m_wk, m_wv, m_wo, m_w_gate, m_w_up, m_w_down, v_wq, v_wk, v_wv, v_wo, v_w_gate, v_w_up, v_w_down):
    weights = dict(zip(NAMES, (wq, wk, wv, wo, w_gate, w_up, w_down), strict=True))

    def take(so_far, sequence):
        h, by_y = sequence
        _, back = jax.vjp(stack, weights, h)
        by_weights, by_h = back(by_y)
        return jax.tree.map(lambda total, term: total + term.astype(jnp.float32), so_far, by_weights), by_h

    none_yet = {name: jnp.zeros(w.shape, jnp.float32) for name, w in weights.items()}
    by_weights, by_x = lax.scan(take, none_yet, (x, dy))
    gradients = [by_weights[name].astype(jnp.bfloat16).astype(jnp.float32) for name in NAMES]
    gradients = clipped(gradients, sum(jnp.sum(g * g) for g in gradients), sum(g.size for g in gradients))
    first = (m_wq, m_wk, m_wv, m_wo, m_w_gate, m_w_up, m_w_down)
    second = (v_wq, v_wk, v_wv, v_wo, v_w_gate, v_w_up, v_w_down)
    new = [adamw(weights[name].astype(jnp.float32), m, v, g) for name, m, v, g in zip(NAMES, first, second, gradients, strict=True)]
    return tuple(one[which] for which in range(3) for one in new)
```

```python
import functools

import jax
import jax.numpy as jnp
from jax import lax
from jax.experimental import pallas as pl
from jax.experimental.pallas import tpu as pltpu
from jax.sharding import PartitionSpec as P

HEAD = 128
THETA = 10000
LOG2E = 1.4426950408889634
HIDDEN = -2e30
SCALE = HEAD**-0.5
E = SCALE * LOG2E
T = 512
HALF = T // 2
FC = 512
VMEM = 60 * 2**20
BF, F32 = jnp.bfloat16, jnp.float32


def dot(a, b):
    return lax.dot_general(a, b, (((1,), (0,)), ((), ())), preferred_element_type=F32)


def dot_nt(a, b):
    return lax.dot_general(a, b, (((1,), (1,)), ((), ())), preferred_element_type=F32)


def dot_tn(a, b):
    return lax.dot_general(a, b, (((0,), (0,)), ((), ())), preferred_element_type=F32)


def rms(x):
    return lax.rsqrt(jnp.mean(x * x, -1, keepdims=True) + 1e-6)


def normed_back(x, dy):
    r = rms(x)
    return r * dy - x * (r * r * r * jnp.mean(x * dy, -1, keepdims=True))


def turn(x, cos, sin):
    return x * cos + pltpu.roll(x, HEAD // 2, 1) * sin


def tables(tokens):
    half = HEAD // 2
    angle = jnp.arange(tokens, dtype=F32)[:, None] * THETA ** (-jnp.arange(half, dtype=F32) / half)
    cos, sin = jnp.cos(angle), jnp.sin(angle)
    return jnp.concatenate([cos, cos], 1), jnp.concatenate([-sin, sin], 1)


def attention_in(i, x_ref, cos_ref, sin_ref, wq_ref, wk_ref, wv_ref, q_ref, k_ref, v_ref, k_s, vt_s, wqkv_s):
    heads = wq_ref.shape[2] // HEAD
    d = wq_ref.shape[2]

    @pl.when(i == 0)
    def _():
        wqkv_s[:, :d] = wq_ref[0]
        wqkv_s[:, d : d + HEAD] = wk_ref[0]
        wqkv_s[:, d + HEAD :] = wv_ref[0]

    x = x_ref[0].astype(F32)
    a = (x * rms(x)).astype(BF)
    cos, sin = cos_ref[...], sin_ref[...]
    qkv = dot(a, wqkv_s[...])
    for n in range(heads):
        one = qkv[:, n * HEAD : (n + 1) * HEAD].astype(BF).astype(F32)
        q_ref[:, n * HEAD : (n + 1) * HEAD] = turn(one, cos, sin).astype(BF)
    k = turn(qkv[:, d : d + HEAD].astype(BF).astype(F32), cos, sin).astype(BF)
    v = qkv[:, d + HEAD :].astype(BF)
    k_ref[...] = k
    v_ref[...] = v
    k_s[pl.ds(pl.multiple_of(i * T, T), T), :] = k
    vt_s[i, :HEAD, :] = v.T
    vt_s[i, HEAD:, :] = jnp.ones((16, T), BF)


def attention_core(i, q_ref, k_s, vt_s, top_s, mix_s, o_ref, lse_ref):
    heads = q_ref.shape[1] // HEAD
    cols = [slice(n * HEAD, (n + 1) * HEAD) for n in range(heads)]
    base = pl.multiple_of(i * T, T)

    k0 = k_s[pl.ds(base, HALF), :]
    v0 = vt_s[i, :, :HALF]
    ok = lax.broadcasted_iota(jnp.int32, (HALF, T), 1) >= lax.broadcasted_iota(jnp.int32, (HALF, T), 0)
    scores = [dot_nt(k0, q_ref[:, c]) for c in cols]
    for n, s in enumerate(scores):
        s = jnp.where(ok, s, HIDDEN)
        top = s.max(axis=0, keepdims=True)
        top_s[n : n + 1, :] = top
        mix_s[n] = dot(v0, jnp.exp2((s - top) * E).astype(BF))
    k1 = k_s[pl.ds(pl.multiple_of(base + HALF, HALF), HALF), :]
    v1 = vt_s[i, :, HALF:]
    scores = [dot_nt(k1, q_ref[HALF:, c]) for c in cols]
    for n, s in enumerate(scores):
        s = jnp.where(ok[:, :HALF], s, HIDDEN)
        old = top_s[n : n + 1, HALF:]
        top = jnp.maximum(old, s.max(axis=0, keepdims=True))
        top_s[n : n + 1, HALF:] = top
        mix_s[n, :, HALF:] = mix_s[n, :, HALF:] * jnp.exp2((old - top) * E) + dot(v1, jnp.exp2((s - top) * E).astype(BF))

    def block(j, _):
        kj = k_s[pl.ds(pl.multiple_of(j * T, T), T), :]
        scores = [dot_nt(kj, q_ref[:, c]) for c in cols]
        weights, keeps = [], []
        for n, s in enumerate(scores):
            old = top_s[n : n + 1, :]
            top = jnp.maximum(old, s.max(axis=0, keepdims=True))
            top_s[n : n + 1, :] = top
            weights.append(jnp.exp2((s - top) * E).astype(BF))
            keeps.append(jnp.exp2((old - top) * E))
        for n in range(heads):
            mix_s[n] = mix_s[n] * keeps[n] + dot(vt_s[j], weights[n])

    lax.fori_loop(0, i, block, None)
    for n, c in enumerate(cols):
        total = mix_s[n, HEAD : HEAD + 1, :]
        o_ref[:, c] = (mix_s[n, :HEAD, :] * (1 / total)).T.astype(BF)
        lse_ref[n : n + 1, :] = top_s[n : n + 1, :] * E + jnp.log2(total)


def after_attention(x_ref, o_ref, wo_ref, h1_ref):
    mixed = dot(o_ref[...], wo_ref[0]).astype(BF)
    h1 = (x_ref[0].astype(F32) + mixed.astype(F32)).astype(BF)
    h1_ref[...] = h1
    return h1.astype(F32)


def first_layer(x_ref, cos_ref, sin_ref, wq_ref, wk_ref, wv_ref, wo_ref, wg_ref, wu_ref, wd_ref,
                q_ref, k_ref, v_ref, o_ref, lse_ref, h1_ref, h2_ref, k_s, vt_s, wqkv_s, top_s, mix_s, act_s):
    i = pl.program_id(0)
    attention_in(i, x_ref, cos_ref, sin_ref, wq_ref, wk_ref, wv_ref, q_ref, k_ref, v_ref, k_s, vt_s, wqkv_s)
    attention_core(i, q_ref, k_s, vt_s, top_s, mix_s, o_ref, lse_ref)
    h1 = after_attention(x_ref, o_ref, wo_ref, h1_ref)
    b = (h1 * rms(h1)).astype(BF)
    for c in range(0, act_s.shape[1], FC):
        gate, up = dot(b, wg_ref[0, :, c : c + FC]), dot(b, wu_ref[0, :, c : c + FC])
        act_s[:, c : c + FC] = (gate * jax.nn.sigmoid(gate) * up).astype(BF)
    out = dot(act_s[...], wd_ref[0]).astype(BF)
    h2_ref[0] = (h1 + out.astype(F32)).astype(BF)


def hidden_back(first, last, me, h1, dy, wg_ref, wu_ref, wd_ref, dh1_ref, pieces, act_s, dg_s, du_s, ag_s, au_s, ad_s):
    b = (h1 * rms(h1)).astype(BF)
    ff = act_s.shape[1]
    for c in range(0, ff, FC):
        here = slice(c, c + FC)
        gate, up = dot(b, wg_ref[0, :, here]), dot(b, wu_ref[0, :, here])
        d_act = dot_nt(dy, wd_ref[0, here, :]).astype(BF).astype(F32)
        sig = jax.nn.sigmoid(gate)
        silu = gate * sig
        act_s[:, here] = (silu * up).astype(BF)
        du_s[:, here] = (d_act * silu).astype(BF)
        dg_s[:, here] = (d_act * up * (sig + silu * (1 - sig))).astype(BF)
    db = dot_nt(dg_s[...], wg_ref[0]) + dot_nt(du_s[...], wu_ref[0])
    dh1_ref[...] = (dy.astype(F32) + normed_back(h1, db)).astype(BF)

    @pl.when(first)
    def _():
        ag_s[...] = jnp.zeros_like(ag_s)
        au_s[...] = jnp.zeros_like(au_s)
        ad_s[...] = jnp.zeros_like(ad_s)

    for c in range(0, ff, FC):
        here = slice(c, c + FC)
        ag_s[:, here] += dot_tn(b, dg_s[:, here])
        au_s[:, here] += dot_tn(b, du_s[:, here])
        ad_s[here, :] += dot_tn(act_s[:, here], dy)

    @pl.when(last)
    def _():
        n = 4
        rows, deep = ag_s.shape[0] // n, ad_s.shape[0] // n
        wide = ad_s.shape[1]
        for rel in range(n):
            owner = lax.rem(me + rel, n)
            put = putter(pieces, rel)
            up_to = 0
            for acc in (ag_s, au_s):
                for c in range(0, ff, wide):
                    put(up_to, acc[pl.ds(pl.multiple_of(owner * rows, rows), rows), c : c + wide].astype(BF))
                    up_to += rows
            put(up_to, ad_s[pl.ds(pl.multiple_of(owner * deep, deep), deep), :].astype(BF))


def putter(pieces, rel):
    half = pieces[1].shape[0]

    def put(row, value):
        count = value.shape[0]
        if rel == 0:
            pieces[0][row : row + count, :] = value
            return
        first, second = pieces[2 * rel - 1], pieces[2 * rel]
        if row < half:
            first[row : min(row + count, half), :] = value[: min(count, half - row)]
        if row + count > half:
            at = max(row, half)
            second[at - half : row + count - half, :] = value[at - row :]

    return put


def last_layer(me_ref, x_ref, cos_ref, sin_ref, wq_ref, wk_ref, wv_ref, wo_ref, wg_ref, wu_ref, wd_ref, dy_ref,
               q_ref, k_ref, v_ref, o_ref, lse_ref, dh1_ref, *rest):
    pieces, (k_s, vt_s, wqkv_s, top_s, mix_s, act_s, dg_s, du_s, ag_s, au_s, ad_s, h1_s) = rest[:7], rest[7:]
    i = pl.program_id(0)
    attention_in(i, x_ref, cos_ref, sin_ref, wq_ref, wk_ref, wv_ref, q_ref, k_ref, v_ref, k_s, vt_s, wqkv_s)
    attention_core(i, q_ref, k_s, vt_s, top_s, mix_s, o_ref, lse_ref)
    h1 = after_attention(x_ref, o_ref, wo_ref, h1_s)
    hidden_back(i == 0, i == pl.num_programs(0) - 1, me_ref[0], h1, dy_ref[0], wg_ref, wu_ref, wd_ref, dh1_ref, pieces,
                act_s, dg_s, du_s, ag_s, au_s, ad_s)


def hidden_layer_back(me_ref, h1_ref, dy_ref, wg_ref, wu_ref, wd_ref, dh1_ref, *rest):
    pieces, (act_s, dg_s, du_s, ag_s, au_s, ad_s) = rest[:7], rest[7:]
    i = pl.program_id(0)
    hidden_back(i == 0, i == pl.num_programs(0) - 1, me_ref[0], h1_ref[...].astype(F32), dy_ref[0], wg_ref, wu_ref, wd_ref, dh1_ref, pieces,
                act_s, dg_s, du_s, ag_s, au_s, ad_s)


def attention_back(me_ref, x_ref, cos_ref, sin_ref, wq_ref, wk_ref, wv_ref, wo_ref, q_ref, k_ref, v_ref, o_ref, lse_ref, dh1_ref, *rest, has_dx):
    rest = list(rest)
    dx_ref = rest.pop(0) if has_dx else None
    pieces, (wqkv_s, do_s, dot_s, qt_s, lse_s, delta_s, p_s, ds_s, dq_s, dkt_s, dvt_s, dqkv_s, aqkv_s, ao_s) = rest[:7], rest[7:]
    step = pl.program_id(0)
    i = pl.num_programs(0) - 1 - step
    d = wq_ref.shape[2]
    heads = d // HEAD
    cols = [slice(n * HEAD, (n + 1) * HEAD) for n in range(heads)]
    side = heads * HALF

    @pl.when(step == 0)
    def _():
        wqkv_s[:, :d] = wq_ref[0]
        wqkv_s[:, d : d + HEAD] = wk_ref[0]
        wqkv_s[:, d + HEAD :] = wv_ref[0]
        aqkv_s[...] = jnp.zeros_like(aqkv_s)
        ao_s[...] = jnp.zeros_like(ao_s)
        dkt_s[...] = jnp.zeros_like(dkt_s)
        dvt_s[...] = jnp.zeros_like(dvt_s)

    dh1 = dh1_ref[...]
    do_s[...] = dot_nt(dh1, wo_ref[0]).astype(BF)
    ao_s[...] += dot_tn(o_ref[...], dh1)
    lse_cols = lse_ref[...].T
    for n, c in enumerate(cols):
        do = do_s[:, c]
        delta = jnp.sum(do.astype(F32) * o_ref[:, c].astype(F32), -1, keepdims=True)
        delta_s[:, c] = jnp.broadcast_to(delta, (T, HEAD))
        lse_s[:, c] = jnp.broadcast_to(lse_cols[:, n : n + 1], (T, HEAD))
        for part in range(2):
            rows = slice(part * HALF, (part + 1) * HALF)
            at = slice(part * side + n * HALF, part * side + (n + 1) * HALF)
            dot_s[:, at] = do[rows].T
            qt_s[:, at] = q_ref[rows, c].T

    def block(j, parts, masked, fresh):
        at = pl.ds(pl.multiple_of(j * HALF, HALF), HALF)
        kj, vj = k_ref[at, :], v_ref[at, :]
        low, high = parts[0] * HALF, (parts[-1] + 1) * HALF
        count = high - low
        if masked:
            ok = lax.broadcasted_iota(jnp.int32, (count, HALF), 0) >= lax.broadcasted_iota(jnp.int32, (count, HALF), 1)
        for n, c in enumerate(cols):
            s, dp = dot_nt(q_ref[low:high, c], kj), dot_nt(do_s[low:high, c], vj)
            lse, delta = (jnp.concatenate([r[low:high, c]] * 2, axis=1) for r in (lse_s, delta_s))
            p = jnp.exp2(s * E - lse)
            if masked:
                p = jnp.where(ok, p, 0.0)
            ds = (p * (dp - delta)).astype(BF)
            p = p.astype(BF)
            for part in parts:
                rows = slice(part * HALF - low, (part + 1) * HALF - low)
                to = slice(part * side + n * HALF, part * side + (n + 1) * HALF)
                p_s[to, :] = p[rows]
                ds_s[to, :] = ds[rows]
            got = dot(ds, kj)
            dq_s[low:high, c] = got if fresh else dq_s[low:high, c] + got
        along = slice(parts[0] * side, (parts[-1] + 1) * side)
        dvt_s[j] += dot(dot_s[:, along], p_s[along, :])
        dkt_s[j] += dot(qt_s[:, along], ds_s[along, :])

    block(2 * i, (0, 1), True, True)
    block(2 * i + 1, (1,), True, False)
    lax.fori_loop(0, 2 * i, lambda j, _: block(j, (0, 1), False, False), None)

    cos, sin = cos_ref[...], -sin_ref[...]
    for c in cols:
        dqkv_s[:, c] = turn(dq_s[:, c] * SCALE, cos, sin).astype(BF)
    for part in range(2):
        rows = slice(part * HALF, (part + 1) * HALF)
        dqkv_s[rows, d : d + HEAD] = turn(dkt_s[2 * i + part].T * SCALE, cos[rows], sin[rows]).astype(BF)
        dqkv_s[rows, d + HEAD :] = dvt_s[2 * i + part].T.astype(BF)
    x = x_ref[0].astype(F32)
    a = (x * rms(x)).astype(BF)
    aqkv_s[...] += dot_tn(a, dqkv_s[...])
    if has_dx:
        da = dot_nt(dqkv_s[...], wqkv_s[...])
        dx_ref[0] = (dh1.astype(F32) + normed_back(x, da)).astype(BF)

    @pl.when(step == pl.num_programs(0) - 1)
    def _():
        n = 4
        rows, deep = aqkv_s.shape[0] // n, ao_s.shape[0] // n
        wide = ao_s.shape[1]
        for rel in range(n):
            owner = lax.rem(me_ref[0] + rel, n)
            put = putter(pieces, rel)
            up_to = 0
            for c in range(0, aqkv_s.shape[1], wide):
                put(up_to, aqkv_s[pl.ds(pl.multiple_of(owner * rows, rows), rows), c : c + wide].astype(BF))
                up_to += rows
            put(up_to, ao_s[pl.ds(pl.multiple_of(owner * deep, deep), deep), :].astype(BF))


def once(shape, layer=None):
    if layer is None:
        return pl.BlockSpec(shape, lambda i, *_: (0,) * len(shape), pipeline_mode=pl.Buffered(1))
    return pl.BlockSpec((1, *shape[1:]), lambda i, *_: (layer, 0, 0), pipeline_mode=pl.Buffered(1))


def params(**more):
    return pltpu.CompilerParams(dimension_semantics=("arbitrary",), vmem_limit_bytes=VMEM, **more)


def rows_spec(width, order):
    return pl.BlockSpec((T, width), lambda i, *_: (order(i), 0))


def states_spec(width, order):
    return pl.BlockSpec((1, T, width), lambda i, *_: (0, order(i), 0))


def struct(shape, dtype=BF):
    return jax.ShapeDtypeStruct(shape, dtype)


def piece_shapes(rows, wide):
    return [struct((rows, wide))] + [struct((rows // 2, wide))] * 6


def pass_forward(layer, me, x, dy, cos, sin, weights):
    wq, wk, wv, wo, wg, wu, wd = weights
    s, width, d, ff = x.shape[1], x.shape[2], wq.shape[2], wg.shape[2]
    up = lambda i: i
    blocks = s // T
    in_specs = [states_spec(width, up), rows_spec(HEAD, up), rows_spec(HEAD, up)] + [once(w.shape, layer) for w in weights]
    given = [x, cos, sin, *weights]
    saved = [struct((s, d)), struct((s, HEAD)), struct((s, HEAD)), struct((s, d)), struct((8, s), F32)]
    saved_specs = [rows_spec(d, up), rows_spec(HEAD, up), rows_spec(HEAD, up), rows_spec(d, up), pl.BlockSpec((8, T), lambda i, *_: (0, i))]
    scratch = [pltpu.VMEM((s, HEAD), BF), pltpu.VMEM((blocks, HEAD + 16, T), BF), pltpu.VMEM((width, d + 2 * HEAD), BF),
               pltpu.VMEM((8, T), F32), pltpu.VMEM((d // HEAD, HEAD + 16, T), F32), pltpu.VMEM((T, ff), BF)]
    flops = 2 * s * width * (2 * d + 2 * HEAD + 3 * ff) + 2 * s * s * d * 2
    if dy is None:
        return pl.pallas_call(
            first_layer,
            grid=(blocks,),
            in_specs=in_specs,
            out_specs=saved_specs + [rows_spec(width, up), states_spec(width, up)],
            out_shape=saved + [struct((s, width)), struct((1, s, width))],
            scratch_shapes=scratch,
            compiler_params=params(),
            cost_estimate=pl.CostEstimate(flops=flops, transcendentals=s * s * 6, bytes_accessed=30 * 2**20),
            name="first_layer",
        )(*given)
    pieces = piece_shapes(3 * width, width)
    return pl.pallas_call(
        last_layer,
        grid_spec=pltpu.PrefetchScalarGridSpec(
            num_scalar_prefetch=1,
            grid=(blocks,),
            in_specs=in_specs + [states_spec(width, up)],
            out_specs=saved_specs + [rows_spec(width, up)] + [once(p.shape) for p in pieces],
            scratch_shapes=scratch + [pltpu.VMEM((T, ff), BF)] * 2
            + [pltpu.VMEM((width, ff), F32)] * 2 + [pltpu.VMEM((ff, width), F32), pltpu.VMEM((T, width), BF)],
        ),
        out_shape=saved + [struct((s, width))] + pieces,
        compiler_params=params(),
        cost_estimate=pl.CostEstimate(flops=2 * flops, transcendentals=s * s * 6, bytes_accessed=40 * 2**20),
        name="last_layer",
    )(me, *given, dy)


def pass_hidden_back(layer, me, h1, dy, wg, wu, wd):
    s, width, ff = h1.shape[0], h1.shape[1], wg.shape[2]
    up = lambda i: i
    pieces = piece_shapes(3 * width, width)
    return pl.pallas_call(
        hidden_layer_back,
        grid_spec=pltpu.PrefetchScalarGridSpec(
            num_scalar_prefetch=1,
            grid=(s // T,),
            in_specs=[rows_spec(width, up), states_spec(width, up)] + [once(w.shape, layer) for w in (wg, wu, wd)],
            out_specs=[rows_spec(width, up)] + [once(p.shape) for p in pieces],
            scratch_shapes=[pltpu.VMEM((T, ff), BF)] * 3 + [pltpu.VMEM((width, ff), F32)] * 2 + [pltpu.VMEM((ff, width), F32)],
        ),
        out_shape=[struct((s, width))] + pieces,
        compiler_params=params(),
        cost_estimate=pl.CostEstimate(flops=2 * s * width * ff * 8, transcendentals=s * ff, bytes_accessed=20 * 2**20),
        name="hidden_back",
    )(me, h1, dy, wg, wu, wd)


def pass_attention_back(layer, me, x, cos, sin, weights, saved, dh1, has_dx):
    wq, wk, wv, wo = weights
    q, k, v, o, lse = saved
    s, width, d = x.shape[1], x.shape[2], wq.shape[2]
    heads, blocks = d // HEAD, s // T
    down = lambda i: blocks - 1 - i
    pieces = piece_shapes((2 * width + d) // 4, width)
    out_specs = [once(p.shape) for p in pieces]
    if has_dx:
        out_specs = [states_spec(width, down)] + out_specs
        pieces = [struct((1, s, width))] + pieces
    side = heads * T
    return pl.pallas_call(
        functools.partial(attention_back, has_dx=has_dx),
        grid_spec=pltpu.PrefetchScalarGridSpec(
            num_scalar_prefetch=1,
            grid=(blocks,),
            in_specs=[states_spec(width, down), rows_spec(HEAD, down), rows_spec(HEAD, down)] + [once(w.shape, layer) for w in weights]
            + [rows_spec(d, down), once(k.shape), once(v.shape), rows_spec(d, down), pl.BlockSpec((8, T), lambda i, *_: (0, down(i))),
               rows_spec(width, down)],
            out_specs=out_specs,
            scratch_shapes=[
                pltpu.VMEM((width, d + 2 * HEAD), BF), pltpu.VMEM((T, d), BF), pltpu.VMEM((HEAD, side), BF), pltpu.VMEM((HEAD, side), BF),
                pltpu.VMEM((T, d), F32), pltpu.VMEM((T, d), F32), pltpu.VMEM((side, HALF), BF), pltpu.VMEM((side, HALF), BF), pltpu.VMEM((T, d), F32),
                pltpu.VMEM((2 * blocks, HEAD, HALF), F32), pltpu.VMEM((2 * blocks, HEAD, HALF), F32), pltpu.VMEM((T, d + 2 * HEAD), BF),
                pltpu.VMEM((width, d + 2 * HEAD), F32), pltpu.VMEM((d, width), F32),
            ],
        ),
        out_shape=pieces,
        compiler_params=params(),
        cost_estimate=pl.CostEstimate(flops=2 * s * s * d * 4 + 2 * s * width * d * 5, transcendentals=s * s * 6, bytes_accessed=20 * 2**20),
        name="attention_back",
    )(me, x, cos, sin, *weights, q, k, v, o, lse, dh1)


def ring(n):
    right = [(i, (i + 1) % n) for i in range(n)]
    left = [(i, (i - 1) % n) for i in range(n)]
    return (lambda t: lax.ppermute(t, "dp", right)), (lambda t: lax.ppermute(t, "dp", left))


def plus(a, b):
    return (a.astype(F32) + b.astype(F32)).astype(BF)


def scatter_sum(pieces, n):
    to_right, to_left = ring(n)
    own, r0, r1, o0, o1, l0, l1 = pieces
    from_left, from_right = to_right(o0), to_left(o1)
    left1, right0 = to_right(r1), to_left(l0)
    left0, right1 = to_right(plus(r0, from_left)), to_left(plus(l1, from_right))
    half = r0.shape[0]
    first = own[:half].astype(F32) + left0.astype(F32) + right0.astype(F32)
    second = own[half:].astype(F32) + left1.astype(F32) + right1.astype(F32)
    return jnp.concatenate([first, second]).astype(BF)


def adamw(w, m, v, g):
    m = 0.9 * m + 0.1 * g
    v = 0.95 * v + 0.05 * g * g
    step = m * lax.rsqrt(v + 1e-8) + 0.1 * w
    return (w - 0.02 * step).astype(BF), m, v


def clipped(gradients, sum_of_squares, count):
    factor = jnp.minimum(1.0, 0.5 * lax.rsqrt(sum_of_squares / count + 1e-30))
    return [g * factor for g in gradients]


def unpack_hidden(g, wide, ff):
    rows = wide // 4
    flat = lambda t: t.reshape(ff // wide, rows, wide).transpose(1, 0, 2).reshape(rows, ff)
    return flat(g[:wide]), flat(g[wide : 2 * wide]), g[2 * wide :]


def unpack_attention(g, wide, d):
    rows = wide // 4
    qkv = g[: 2 * rows].reshape(2, rows, wide).transpose(1, 0, 2).reshape(rows, 2 * wide)
    return qkv[:, :d], qkv[:, d : d + HEAD], qkv[:, d + HEAD :], g[2 * rows :]


def solution(mesh):
    n = mesh.shape["dp"]

    def step(x, dy, *arrays):
        weights, m, v = (arrays[i : i + 7] for i in (0, 7, 14))
        me = lax.axis_index("dp")
        me1 = me[None].astype(jnp.int32)
        cos, sin = tables(x.shape[1])
        attn, hidden = weights[:4], weights[4:]
        *saved0, h1, h = pass_forward(0, me1, x, None, cos, sin, weights)
        *saved1, dh1 = (last := pass_forward(1, me1, h, dy, cos, sin, weights))[:6]
        g_hidden1 = scatter_sum(last[6:], n)
        dh, *pieces = pass_attention_back(1, me1, h, cos, sin, attn, saved1, dh1, True)
        g_attn1 = scatter_sum(pieces, n)
        dh1, *pieces = pass_hidden_back(0, me1, h1, dh, *hidden)
        g_hidden0 = scatter_sum(pieces, n)
        pieces = pass_attention_back(0, me1, x, cos, sin, attn, saved0, dh1, False)
        g_attn0 = scatter_sum(pieces, n)

        wide, d, ff = weights[0].shape[1], weights[0].shape[2], hidden[0].shape[2]
        by_layer = [(*unpack_attention(a, wide, d), *unpack_hidden(b, wide, ff)) for a, b in ((g_attn0, g_hidden0), (g_attn1, g_hidden1))]
        gradients = [jnp.stack([one[i] for one in by_layer]).astype(F32) for i in range(7)]
        squares = lax.psum(sum(jnp.sum(g * g) for g in gradients), "dp")
        gradients = clipped(gradients, squares, lax.psum(1, "dp") * sum(g.size for g in gradients))
        own = [lax.dynamic_slice_in_dim(w, me * one.shape[1], one.shape[1], 1).astype(F32) for w, one in zip(weights, m, strict=True)]
        new = [adamw(w, m, v, g) for w, m, v, g in zip(own, m, v, gradients, strict=True)]
        whole = [lax.all_gather(one[0], "dp", axis=1, tiled=True) for one in new]
        return (*whole, *(one[1] for one in new), *(one[2] for one in new))

    states, all_of, cut = P(("rep", "dp"), None, None), P(None, None, None), P(None, "dp", None)
    return jax.shard_map(
        step,
        mesh=mesh,
        in_specs=(states, states) + (all_of,) * 7 + (cut,) * 14,
        out_specs=(P("rep", None, None),) * 7 + (P("rep", "dp", None),) * 14,
        check_vma=False,
    )
```

```python
import functools

import jax
import jax.numpy as jnp
import numpy as np
from jax import lax
from jax.experimental import pallas as pl
from jax.experimental.pallas import tpu as pltpu
from jax.sharding import PartitionSpec as P


N = 4
HEAD = 128
THETA = 10000
LOG2E = 1.4426950408889634
HIDDEN = -2e30
SCALE = HEAD**-0.5
E = SCALE * LOG2E
T = 512
HALVES = 2
PIECE = 256
HALF = T // HALVES
LOW = 64
VMEM = 62 * 2**20
BF, F32 = jnp.bfloat16, jnp.float32
MESH = pl.DeviceIdType.MESH
ANY = pl.BlockSpec(memory_space=pl.ANY)
FIRST = 0
NEXT = 1


def dot(a, b, ca=NEXT, cb=FIRST):
    return lax.dot_general(a, b, (((ca,), (cb,)), ((), ())), preferred_element_type=F32)


def dot_nt(a, b):
    return dot(a, b, NEXT, NEXT)


def dot_tn(a, b):
    return dot(a, b, FIRST, FIRST)


def rms(x):
    return lax.rsqrt(jnp.mean(x * x, -NEXT, keepdims=True) + 1e-6)


def normed(x):
    return (x * rms(x)).astype(BF)


def sigmoid(x):
    return 0.5 * jnp.tanh(0.5 * x) + 0.5


def normed_back(x, dy):
    r = rms(x)
    return r * dy - x * (r * r * r * jnp.mean(x * dy, -NEXT, keepdims=True))


def plus(*terms):
    return functools.reduce(lambda a, b: a + b, [t.astype(F32) for t in terms])


def rows_in(a):
    return a.shape[-HALVES]


def lanes(a):
    return a.shape[-NEXT]


def block(i, size):
    return pl.ds(pl.multiple_of(i * size, size), size)


def turn(x, cos, sin):
    return x * cos + pltpu.roll(x, HEAD // HALVES, NEXT) * sin


def tables(tokens):
    half = HEAD // HALVES
    rate = float(THETA) ** (-np.arange(half) / half)

    def at(places):
        angle = places[:, None] * rate
        cos, sin = np.cos(angle), np.sin(angle)
        return jnp.asarray(np.stack([np.concatenate([cos, cos], NEXT), np.concatenate([-sin, sin], NEXT)]), F32)

    return at(np.arange(LOW)), at(np.arange(FIRST, tokens, LOW))


def angles(low_ref, high_ref):
    (cos, sin), (cos_high, sin_high) = low_ref[:], high_ref[:][:, :, None]
    return (cos_high * cos - sin_high * sin).reshape(T, HEAD), (sin_high * cos + cos_high * sin).reshape(T, HEAD)


def heads_of(width):
    return [slice(at, at + HEAD) for at in range(FIRST, width, HEAD)]


def side_by_side(out, *refs):
    at = FIRST
    for ref in refs:
        wide = lanes(ref)
        out[:, at : at + wide] = ref[FIRST]
        at += wide


def attention_forward(i, x_ref, low_ref, high_ref, wq_ref, wk_ref, wv_ref, q_ref, k_ref, v_ref, o_ref, lse_ref, k_s, vt_s, wqkv_s, top_s, mix_s, between):
    d = lanes(wq_ref)
    cols = heads_of(d)
    pl.when(i == FIRST)(lambda: side_by_side(wqkv_s, wq_ref, wk_ref, wv_ref))
    cos, sin = angles(low_ref, high_ref)
    qkv = dot(normed(x_ref[FIRST].astype(F32)), wqkv_s[:]).astype(BF)
    for c in cols:
        q_ref[:, c] = turn(qkv[:, c].astype(F32), cos, sin).astype(BF)
    k = turn(qkv[:, d : d + HEAD].astype(F32), cos, sin).astype(BF)
    v = qkv[:, d + HEAD :]
    k_ref[:] = k
    v_ref[:] = v
    k_s[block(i, T), :] = k
    vt_s[i, :HEAD, :] = v.T
    vt_s[i, HEAD:, :] = jnp.ones_like(vt_s[i, HEAD:, :])

    if between:
        between()
    ok = lax.broadcasted_iota(jnp.int32, (HALF, T), NEXT) >= lax.broadcasted_iota(jnp.int32, (HALF, T), FIRST)
    k0, v0 = k_s[block(HALVES * i, HALF), :], vt_s[i, :, :HALF]
    scores = [dot_nt(k0, q_ref[:, c]) for c in cols]
    for n, s in enumerate(scores):
        s = jnp.where(ok, s, HIDDEN)
        top = s.max(axis=FIRST, keepdims=True)
        top_s[n : n + NEXT, :] = top
        mix_s[n] = dot(v0, jnp.exp2((s - top) * E).astype(BF))
    k1, v1 = k_s[block(HALVES * i + NEXT, HALF), :], vt_s[i, :, HALF:]
    scores = [dot_nt(k1, q_ref[HALF:, c]) for c in cols]
    for n, s in enumerate(scores):
        s = jnp.where(ok[:, :HALF], s, HIDDEN)
        old = top_s[n : n + NEXT, HALF:]
        top = jnp.maximum(old, s.max(axis=FIRST, keepdims=True))
        top_s[n : n + NEXT, HALF:] = top
        mix_s[n, :, HALF:] = mix_s[n, :, HALF:] * jnp.exp2((old - top) * E) + dot(v1, jnp.exp2((s - top) * E).astype(BF))

    def earlier(j, _):
        kj = k_s[block(j, T), :]
        scores = [dot_nt(kj, q_ref[:, c]) for c in cols]
        weights, keeps = [], []
        for n, s in enumerate(scores):
            old = top_s[n : n + NEXT, :]
            top = jnp.maximum(old, s.max(axis=FIRST, keepdims=True))
            top_s[n : n + NEXT, :] = top
            weights.append(jnp.exp2((s - top) * E).astype(BF))
            keeps.append(jnp.exp2((old - top) * E))
        for n, (weight, keep) in enumerate(zip(weights, keeps)):
            mix_s[n] = mix_s[n] * keep + dot(vt_s[j], weight)

    lax.fori_loop(FIRST, i, earlier, None)
    for n, c in enumerate(cols):
        total = mix_s[n, HEAD : HEAD + NEXT, :]
        o_ref[c, :] = (mix_s[n, :HEAD, :] * (NEXT / total)).astype(BF)
        lse_ref[n : n + NEXT, :] = top_s[n : n + NEXT, :] * E + jnp.log2(total)


def forward(x_ref, low_ref, high_ref, wq_ref, wk_ref, wv_ref, *refs, layer, whole, plan):
    given, refs = (refs[:4], refs[4:]) if whole else (refs[:NEXT], refs[NEXT:])
    letters, refs = refs[: plan[FIRST]], refs[plan[FIRST] :]
    saved, h1_ref, refs = refs[:5], refs[5], refs[6:]
    h2_ref, refs = (refs[FIRST], refs[NEXT:]) if whole else (None, refs)
    arrived, refs = refs[: len(plan[NEXT])], refs[len(plan[NEXT]) :]
    scratch, held, (act_s, sem) = refs[:5], refs[5 : 5 + len(given)], refs[-4:-HALVES]
    post = Post(plan[HALVES](letters, arrived), *refs[-HALVES:])
    i = pl.program_id(FIRST)
    loads = [pltpu.make_async_copy(src.at[layer], dst, sem.at[k]) for k, (src, dst) in enumerate(zip(given, held))]

    @pl.when(i == FIRST)
    def _():
        greet_all()
        for copy in loads:
            copy.start()

    def between():
        @pl.when(i == FIRST)
        def _():
            greeted()
            post.start()

    if whole:
        between()
    attention_forward(i, x_ref, low_ref, high_ref, wq_ref, wk_ref, wv_ref, *saved, *scratch, None if whole else between)

    @pl.when(i == FIRST)
    def _():
        for copy in loads:
            copy.wait()

    o_ref = saved[3]
    h1 = plus(x_ref[FIRST], dot_tn(o_ref[:], held[FIRST][:]).astype(BF)).astype(BF)
    h1_ref[:] = h1
    if whole:
        _, wg, wu, wd = held
        b = normed(h1.astype(F32))
        for c in range(FIRST, lanes(act_s), T):
            here = slice(c, c + T)
            gate, up = dot(b, wg[:, here]), dot(b, wu[:, here])
            act_s[:, here] = (gate * sigmoid(gate) * up).astype(BF)
        h2_ref[FIRST] = plus(h1_ref[:], dot(act_s[:], wd[:]).astype(BF)).astype(BF)
    pl.when(i == pl.num_programs(FIRST) - NEXT)(post.finish)


def place(step):
    return {"dp": lax.rem(lax.axis_index("dp") + step, N)}


def greet(steps=(NEXT, N - NEXT)):
    for step in steps:
        pl.semaphore_signal(pltpu.get_barrier_semaphore(), inc=NEXT, device_id=place(step), device_id_type=MESH)


def greeted(count=3):
    pl.semaphore_wait(pltpu.get_barrier_semaphore(), count)


class Post:
    def __init__(self, copies, send, recv):
        self.copies, self.send, self.recv = copies, send, recv

    def each(self, act):
        rep = lax.axis_index("rep")
        core = lax.rem(rep, HALVES)
        ways = {"right": place(NEXT), "left": place(N - NEXT), "other": {"rep": rep + NEXT - HALVES * core}}
        for k, (src, dst, way) in enumerate(self.copies):
            for n, one in enumerate(src if isinstance(src, tuple) else (src,)):
                copy = pltpu.make_async_remote_copy(src_ref=one, dst_ref=dst, send_sem=self.send.at[k], recv_sem=self.recv.at[k], device_id=ways[way],
                                                    device_id_type=MESH)
                if isinstance(src, tuple):
                    pl.when(core == n)(functools.partial(act, copy))
                else:
                    act(copy)

    def start(self):
        self.each(lambda copy: copy.start())

    def finish(self):
        self.each(lambda copy: copy.wait_recv())
        self.each(lambda copy: copy.wait_send())

    @staticmethod
    def scratch(plan):
        return [pltpu.SemaphoreType.DMA((plan[-NEXT],))] * HALVES


def greet_all():
    rep = lax.axis_index("rep")
    greet()
    pl.semaphore_signal(pltpu.get_barrier_semaphore(), inc=NEXT, device_id={"rep": rep + NEXT - HALVES * lax.rem(rep, HALVES)}, device_id_type=MESH)


class Ring:
    def __init__(self, pieces, scratch, fetched=None):
        self.own, self.right, self.left, self.right0, self.left1 = pieces
        self.from_left, self.from_right, self.then_left, self.then_right, self.send, self.recv = scratch[:6]
        self.loads = []
        if fetched:
            local = fetched[-NEXT]
            pairs = zip((self.own, self.right0, self.left1), fetched)
            self.loads = [pltpu.make_async_copy(src, dst, local.at[k]) for k, (src, dst) in enumerate(pairs)]
            self.own, self.right0, self.left1 = fetched[:-NEXT]
        self.half = rows_in(self.right0)

    @staticmethod
    def scratch(rows, wide):
        return [pltpu.VMEM((rows, wide), BF)] * HALVES + [pltpu.VMEM((rows // HALVES, wide), BF)] * HALVES + [pltpu.SemaphoreType.DMA((6,))] * HALVES

    @staticmethod
    def fetched(rows, wide):
        return [pltpu.VMEM((rows, wide), BF)] + [pltpu.VMEM((rows // HALVES, wide), BF)] * HALVES + [pltpu.SemaphoreType.DMA((3,))]

    def remote(self, k):
        top, low = pl.ds(FIRST, self.half), pl.ds(self.half, self.half)
        src, dst, half = (
            (self.right, self.from_left, top), (self.left, self.from_right, low), (self.right, self.from_left, low), (self.left, self.from_right, top),
            (self.right0, self.then_left, None), (self.left1, self.then_right, None),
        )[k]
        if half is not None:
            src, dst = src.at[half], dst.at[half]
        return pltpu.make_async_remote_copy(src_ref=src, dst_ref=dst, send_sem=self.send.at[k], recv_sem=self.recv.at[k],
                                            device_id=place(N - NEXT if k % HALVES else NEXT), device_id_type=MESH)

    def start(self):
        for copy in self.loads:
            copy.start()
        for k in range(N):
            self.remote(k).start()

    def go_on(self):
        for copy in self.loads:
            copy.wait()
        for k in (FIRST, NEXT):
            self.remote(k).wait_recv()
        half = self.half
        self.right0[:] = plus(self.right0[:], self.from_left[:half, :]).astype(BF)
        self.left1[:] = plus(self.left1[:], self.from_right[half:, :]).astype(BF)

    def second(self):
        for k in (N, N + NEXT):
            self.remote(k).start()

    def finish(self, out, row, squares):
        for k in range(HALVES, N + HALVES):
            self.remote(k).wait_recv()
        half, own = self.half, self.own
        rows = half if half % 96 else 96
        for base, left, right in ((FIRST, (self.then_left, FIRST), (self.from_right, FIRST)), (half, (self.from_left, half), (self.then_right, FIRST))):

            def some(c, _):
                at = pl.multiple_of(c * rows, 32)
                terms = [ref[pl.ds(start + at, rows), :] for ref, start in ((own, base), left, right)]
                total = plus(*terms).astype(BF)
                out[pl.ds(row + base + at, rows), :] = total
                wide = total.astype(F32)
                squares[:] += (wide * wide).reshape(rows // 8, 8, lanes(wide)).sum(FIRST)

            lax.fori_loop(FIRST, half // rows, some, None)
        for k in range(N + HALVES):
            self.remote(k).wait_send()


def put(pieces, step, row, value):
    own, right, left, right0, left1 = pieces
    half = rows_in(right0)
    homes = (((own, FIRST), (own, half)), ((right0, FIRST), (right, half)), ((right, FIRST), (left, half)), ((left, FIRST), (left1, FIRST)))[step]
    for base, (ref, at) in zip((FIRST, half), homes):
        start, end = max(row, base), min(row + rows_in(value), base + half)
        if start < end:
            ref[at + start - base : at + end - base, :] = value[start - row : end - row]


def piece_shapes(rows, wide):
    return [(rows, wide)] * 3 + [(rows // HALVES, wide)] * HALVES


def hidden_back(h1_hbm, dy_hbm, ot_hbm, wg_hbm, wu_hbm, wd_hbm, *refs, layer, incoming, quarters, plan):
    sent, refs = refs[: 5 * incoming], refs[5 * incoming :]
    letters, refs = refs[: plan[FIRST]], refs[plan[FIRST] :]
    n = NEXT + quarters + incoming
    (dh1_ref, *sums), squares, out_pieces, refs = refs[:n], refs[n], refs[n + NEXT : n + 6], refs[n + 6 :]
    post = Post(plan[HALVES](letters, refs[: len(plan[NEXT])]), *refs[-HALVES:])
    refs = refs[len(plan[NEXT]) : -HALVES]
    h1_s, dy_s, ot_s, wg_s, wu_s, wd_s, b_s, bt_s, db_s, dg_s, du_s, act_s, ag_s, au_s, ad_s, ao_s, load_sem = refs[:17]
    refs = refs[17:]
    rings, pieces = [], []
    for _ in range(quarters):
        pieces.append(refs[:5])
        rings.append(Ring(refs[:5], refs[5:11]))
        refs = refs[11:]
    late = Ring(sent, refs[:6], refs[6:]) if incoming else None
    blocks = rows_in(h1_s) // T
    part = lanes(wg_s) // N
    steps = N * blocks

    def token_loads(i):
        return [pltpu.make_async_copy(src.at[block(i, T)], dst.at[block(i, T)], load_sem.at[i, k])
                for k, (src, dst) in enumerate(((h1_hbm, h1_s), (dy_hbm.at[FIRST], dy_s)))]

    ot_load = pltpu.make_async_copy(ot_hbm, ot_s, load_sem.at[FIRST, HALVES])

    def weight_loads(c):
        copies = []
        for r in range(N):
            there, here = pl.ds((r * N + c) * part, part), pl.ds(r * part, part)
            copies += [pltpu.make_async_copy(wg_hbm.at[layer, :, there], wg_s.at[c, :, here], load_sem.at[N + c, r]),
                       pltpu.make_async_copy(wu_hbm.at[layer, :, there], wu_s.at[c, :, here], load_sem.at[N + c, N + r]),
                       pltpu.make_async_copy(wd_hbm.at[layer, there, :], wd_s.at[c, here, :], load_sem.at[N + c, HALVES * N + r])]
        return copies

    greet_all()
    for i in range(N):
        for copy in token_loads(i) + weight_loads(i):
            copy.start()
    ot_load.start()
    for ref in (squares, db_s, ag_s, au_s, ad_s, dg_s, du_s, act_s):
        ref[:] = jnp.zeros_like(ref)

    def events(t):
        for k in range(N):

            @pl.when(t == k)
            def _():
                for copy in token_loads(k):
                    copy.wait()
                b = normed(h1_s[block(k, T), :].astype(F32))
                b_s[block(k, T), :] = b
                bt_s[k] = b.T

            @pl.when(t == k * blocks)
            def _():
                for copy in weight_loads(k):
                    copy.wait()

        pl.when(t == FIRST)(greeted)
        if incoming:
            for at, act in ((FIRST, late.start), (N, late.go_on), (N, late.second), (11, lambda: late.finish(sums[-NEXT], FIRST, squares))):
                pl.when(t == at)(act)
        pl.when(t == FIRST)(post.start)
        for k, ring in enumerate(rings):
            at = (k + NEXT) * blocks + NEXT
            for when, act in ((at, ring.start), ((10, 13)[k], ring.go_on), ((10, 13)[k], ring.second), ((15, steps)[k], functools.partial(ring.finish, sums[k], FIRST, squares))):
                if when < steps:
                    pl.when(t == when)(act)

    def products(t):
        i, c, slot = lax.rem(t, blocks), lax.div(t, blocks), lax.rem(t, HALVES)
        b, dy = b_s[block(i, T), :], dy_s[block(i, T), :]
        for at in range(FIRST, lanes(wg_s), PIECE):
            here = slice(at, at + PIECE)
            gate, up, d_act = dot(b, wg_s[c, :, here]), dot(b, wu_s[c, :, here]), dot_nt(dy, wd_s[c, here, :])
            sig = sigmoid(gate)
            silu = gate * sig
            act_s[slot, :, here] = (silu * up).astype(BF)
            du_s[slot, :, here] = (d_act * silu).astype(BF)
            dg_s[slot, :, here] = (d_act * up * (sig + silu * (NEXT - sig))).astype(BF)

    def add_up(t, slot):
        i, c = lax.rem(t, blocks), lax.div(t, blocks)
        dg, du, act = dg_s[slot], du_s[slot], act_s[slot]
        ag_s[:] += dot(bt_s[i], dg)
        au_s[:] += dot(bt_s[i], du)
        ad_s[:] += dot_tn(act, dy_s[block(i, T), :])
        db_s[block(i, T), :] += dot_nt(dg, wg_s[c]) + dot_nt(du, wu_s[c])

    def emit(k):
        for step in range(N):
            mine = block(lax.rem(lax.axis_index("dp") + step, N), part)
            for m, acc in enumerate((ag_s, au_s, ad_s)):
                to, row = (pieces[k], FIRST) if k < quarters else (out_pieces, (k - quarters) * 3 * part)
                put(to, step, row + m * part, acc[mine, :].astype(BF))
        if k < N - NEXT:
            for acc in (ag_s, au_s, ad_s):
                acc[:] = jnp.zeros_like(acc)

    def close(t):
        rows = block(lax.rem(t, blocks), T)
        dh1 = plus(dy_s[rows, :], normed_back(h1_s[rows, :].astype(F32), db_s[rows, :])).astype(BF)
        dh1_ref[rows, :] = dh1

    def step(t, _):
        events(t)
        before = jnp.maximum(t - NEXT, FIRST)
        add_up(before, NEXT - lax.rem(t, HALVES))
        products(t)
        for k in range(N - NEXT):
            pl.when(t == (k + NEXT) * blocks)(functools.partial(emit, k))
        pl.when(t > steps - blocks)(lambda: close(before))

    lax.fori_loop(FIRST, steps, step, None)
    add_up(steps - NEXT, NEXT)
    close(steps - NEXT)
    ot_load.wait()
    ao_s[:] = dot(ot_s[:], dh1_ref[:])
    emit(N - NEXT)
    deep = rows_in(ao_s) // N
    for step in range(N):
        put(out_pieces, step, (N - quarters) * 3 * part, ao_s[block(lax.rem(lax.axis_index("dp") + step, N), deep), :].astype(BF))
    rings[-NEXT].finish(sums[quarters - NEXT], FIRST, squares)
    post.finish()


def attention_back(x_ref, low_ref, high_ref, wq_ref, wk_ref, wv_ref, wo_ref, q_ref, k_ref, v_ref, ot_ref, lse_ref, dh1_ref, *refs, has_dx, plan, parts, count):
    sent, letters, refs = refs[:5], refs[5 : 5 + plan[FIRST]], refs[5 + plan[FIRST] :]
    before, refs = refs[:parts], refs[parts:]
    dx_ref, refs = (refs[FIRST], refs[NEXT:]) if has_dx else (None, refs)
    if has_dx:
        sums, squares, pieces, refs = refs[FIRST], refs[NEXT], refs[HALVES:7], refs[7:]
    else:
        given, (sums, own_sum, factor_ref), refs = before, refs[:3], refs[3:]
        pieces, tail, squares, all_s, part_send, part_recv = refs[-17:-12], refs[-12:-6], *refs[-6:-HALVES]
        refs = (*refs[:-17], *refs[-HALVES:])
    post = Post(plan[HALVES](letters, refs[: len(plan[NEXT])]), *refs[-HALVES:])
    refs = refs[len(plan[NEXT]) : -HALVES]
    wqkv_s, dot_s, qt_s, qx_s, dox_s, kx_s, vx_s, kr_s, dq_s, dkt_s, dvt_s, dqkv_s, aqkv_s = refs[:13]
    ring = Ring(sent, refs[13:19], refs[19:23])
    step, last = pl.program_id(FIRST), pl.num_programs(FIRST) - NEXT
    i = last - step
    d = lanes(wq_ref)
    cols = heads_of(d)
    side = len(cols) * HALF

    @pl.when(step == FIRST)
    def _():
        if has_dx:
            greet_all()
        else:
            greet(range(NEXT, N))
        side_by_side(wqkv_s, wq_ref, wk_ref, wv_ref)
        for ref in (aqkv_s, dkt_s, dvt_s, squares, qx_s, dox_s):
            ref[:] = jnp.zeros_like(ref)
        less = jnp.where(lax.broadcasted_iota(jnp.int32, k_ref.shape, NEXT) < 3, -1.0, 0.0).astype(BF)
        kx_s[:] = jnp.concatenate([k_ref[:], less], NEXT)
        vx_s[:] = jnp.concatenate([v_ref[:], less], NEXT)
        kr_s[:] = jnp.concatenate([k_ref[:], pltpu.roll(k_ref[:].astype(F32), HEAD // HALVES, NEXT).astype(BF)], NEXT)

    dh1 = dh1_ref[:]
    do = dot_nt(dh1, wo_ref[FIRST]).astype(BF)
    dot_all = dot_nt(wo_ref[FIRST], dh1).astype(BF)
    for n, c in enumerate(cols):
        delta = jnp.sum(dot_all[c, :].astype(F32) * ot_ref[c, :].astype(F32), FIRST, keepdims=True)
        for value, ref in ((lse_ref[n : n + NEXT, :] * (NEXT / E), qx_s), (delta, dox_s)):
            three = []
            for _ in range(3):
                three.append(value.astype(BF).astype(F32))
                value = value - three[-NEXT]
            three = jnp.concatenate(three + [jnp.zeros((5, T), F32)], FIRST).T.astype(BF)
            for part in range(HALVES):
                ref[block(part * len(cols) + n, HALF), HEAD : HEAD + 8] = three[part * HALF : (part + NEXT) * HALF]
        for part in range(HALVES):
            rows = slice(part * HALF, (part + NEXT) * HALF)
            at = slice(part * side + n * HALF, part * side + (n + NEXT) * HALF)
            q = q_ref[rows, c]
            qx_s[at, :HEAD] = q
            dox_s[at, :HEAD] = do[rows, c]
            qt_s[:, at] = q.T
            dot_s[:, at] = dot_all[c, rows]

    @pl.when(step == FIRST)
    def _():
        greeted()
        ring.start()

    pl.when(step == NEXT)(ring.go_on)

    def keys(j, first, masked, fresh):
        at, along = block(j, HALF), slice(first * side, HALVES * side)
        p = jnp.exp2(dot_nt(qx_s[along, :], kx_s[at, :]) * E)
        if masked:
            ok = lax.broadcasted_iota(jnp.int32, (HALF, HALF), FIRST) >= lax.broadcasted_iota(jnp.int32, (HALF, HALF), NEXT)
            cut = jnp.where(ok[None], p[:side].reshape(-NEXT, HALF, HALF), 0.0).reshape(side, HALF)
            p = cut if first else jnp.concatenate([cut, p[side:]], FIRST)
        ds = (p * dot_nt(dox_s[along, :], vx_s[at, :])).astype(BF)
        p = p.astype(BF)
        got = dot(ds, kr_s[at, :])
        dq_s[along, :] = got if fresh else dq_s[along, :] + got
        dvt_s[j] += dot(dot_s[:, along], p)
        dkt_s[j] += dot(qt_s[:, along], ds)

    keys(HALVES * i, FIRST, True, True)
    keys(HALVES * i + NEXT, NEXT, True, False)
    pl.when(step == NEXT)(ring.second)
    pl.when(step == NEXT)(post.start)

    def earlier(j, _):
        for half in range(HALVES):
            keys(HALVES * j + half, FIRST, False, False)

    lax.fori_loop(FIRST, i, earlier, None)

    cos, sin = angles(low_ref, high_ref)
    sin = -sin
    for part in range(HALVES):
        rows = slice(part * HALF, (part + NEXT) * HALF)
        for n, c in enumerate(cols):
            dq = dq_s[block(part * len(cols) + n, HALF), :] * SCALE
            dqkv_s[rows, c] = (dq[:, :HEAD] * cos[rows] + dq[:, HEAD:] * sin[rows]).astype(BF)
        dqkv_s[rows, d : d + HEAD] = turn(dkt_s[HALVES * i + part].T * SCALE, cos[rows], sin[rows]).astype(BF)
        dqkv_s[rows, d + HEAD :] = dvt_s[HALVES * i + part].T.astype(BF)
    x = x_ref[FIRST].astype(F32)
    aqkv_s[:] += dot_tn(normed(x), dqkv_s[:])
    if has_dx:
        dx_ref[FIRST] = plus(dh1, normed_back(x, dot_nt(dqkv_s[:], wqkv_s[:]))).astype(BF)

    @pl.when(step == last)
    def _():
        rows, wide = rows_in(aqkv_s) // N, lanes(squares)
        for place in range(N):
            owner = lax.rem(lax.axis_index("dp") + place, N)
            for k, c in enumerate(range(FIRST, lanes(aqkv_s), wide)):
                put(pieces, place, k * rows, aqkv_s[block(owner, rows), c : c + wide].astype(BF))
        if has_dx:
            ring.finish(sums, FIRST, squares)
            post.finish()
        else:
            finish_all(ring, Ring(pieces, tail), sums, own_sum, squares, given, factor_ref, all_s, part_send, part_recv, count)
            post.finish()


def finish_all(ring, last, sums, last_sum, squares, given, factor_ref, all_s, part_send, part_recv, count):
    others = range(NEXT, N)
    me = lax.axis_index("dp")
    last.start()
    ring.finish(sums, FIRST, squares)
    squares[:] = plus(squares[:], *(ref[:] for ref in given))
    last.go_on()
    last.second()
    last.finish(last_sum, FIRST, squares)
    acc = squares[:]
    all_s[me] = plus(*(acc[:, c] for c in heads_of(lanes(acc))))

    def send(step):
        return pltpu.make_async_remote_copy(src_ref=all_s.at[me], dst_ref=all_s.at[me], send_sem=part_send.at[step - NEXT], recv_sem=part_recv.at[step - NEXT],
                                            device_id=place(step), device_id_type=MESH)

    for step in others:
        send(step).start()
    for step in others:
        send(step).wait_recv()
    total = jnp.sum(plus(*(all_s[k] for k in range(N))), keepdims=True)
    factor_ref[:] = jnp.broadcast_to(jnp.minimum(1.0, 0.5 * lax.rsqrt(total * (NEXT / count) + 1e-30)), factor_ref.shape)
    for step in others:
        send(step).wait_send()


def up(i):
    return i


def once(shape, layer=None):
    if layer is None:
        return pl.BlockSpec(shape, lambda i, *_: (FIRST,) * len(shape), pipeline_mode=pl.Buffered(NEXT))
    return pl.BlockSpec((NEXT, *shape[NEXT:]), lambda i, *_: (layer, FIRST, FIRST), pipeline_mode=pl.Buffered(NEXT))


def params(**more):
    return pltpu.CompilerParams(dimension_semantics=("arbitrary",), vmem_limit_bytes=VMEM, **more)


def talking(collective_id):
    return params(collective_id=collective_id, has_side_effects=True)


def cost(flops, megabytes):
    return pl.CostEstimate(flops=int(flops), transcendentals=FIRST, bytes_accessed=megabytes * HALVES**20)


def rows_spec(width, order=up):
    return pl.BlockSpec((T, width), lambda i, *_: (order(i), FIRST))


def columns_spec(rows, order=up):
    return pl.BlockSpec((rows, T), lambda i, *_: (FIRST, order(i)))


def states_spec(width, order=up):
    return pl.BlockSpec((NEXT, T, width), lambda i, *_: (FIRST, order(i), FIRST))


def angle_specs(order=up):
    return once((HALVES, LOW, HEAD)), pl.BlockSpec((HALVES, T // LOW, HEAD), lambda i, *_: (FIRST, order(i), FIRST))


def struct(shape, dtype=BF):
    return jax.ShapeDtypeStruct(shape, dtype)


def structs(shapes):
    return [struct(shape) for shape in shapes]


def scratches(*shapes, dtype=BF):
    return [pltpu.VMEM(shape, dtype) for shape in shapes]


def pass_forward(layer, x, low, high, weights, letters, plan, collective_id):
    wq, *_, wo = weights[:4]
    s, width, d = rows_in(x), lanes(x), lanes(wq)
    blocks, heads = s // T, d // HEAD
    streamed = weights[3:]
    ff = rows_in(weights[-NEXT])
    whole = len(streamed) > NEXT
    return pl.pallas_call(
        functools.partial(forward, layer=layer, whole=whole, plan=plan),
        grid=(blocks,),
        in_specs=[states_spec(width), *angle_specs()] + [once(w.shape, layer) for w in weights[:3]] + [ANY] * (len(streamed) + plan[FIRST]),
        out_specs=[rows_spec(d), rows_spec(HEAD), rows_spec(HEAD), columns_spec(d), columns_spec(8), rows_spec(width)] + [states_spec(width)] * whole + [ANY] * len(plan[NEXT]),
        out_shape=structs([(s, d), (s, HEAD), (s, HEAD), (d, s)]) + [struct((8, s), F32)] + structs([(s, width)] + [x.shape] * whole) + plan[NEXT],
        scratch_shapes=scratches((s, HEAD), (blocks, HEAD + 16, T), (width, d + HALVES * HEAD)) + scratches((8, T), (heads, HEAD + 16, T), dtype=F32)
        + scratches(*(w.shape[NEXT:] for w in streamed), (T, ff)) + [pltpu.SemaphoreType.DMA((len(streamed),))] + Post.scratch(plan),
        compiler_params=talking(collective_id),
        cost_estimate=cost(HALVES * s * (width * (HALVES * d + HALVES * HEAD + 3 * ff * whole) + s * d), 30),
    )(x, low, high, *weights, *letters)


def pass_hidden_back(layer, h1, dy, ot, wg, wu, wd, sent, letters, plan, collective_id):
    s, width, ff = rows_in(h1), lanes(h1), lanes(wg)
    quarters, part = N // HALVES, ff // N
    packed = 3 * part // N
    incoming = NEXT if sent else FIRST
    whole, blocks = part, s // T
    sums = [(packed, width)] * quarters + [sent[FIRST].shape] * incoming if sent else [(packed, width)] * quarters
    pieces = piece_shapes(quarters * packed + rows_in(ot) // N, width)
    scratch = scratches((s, width), (s, width), ot.shape, (N, width, whole), (N, width, whole), (N, whole, width), (s, width), (blocks, width, T))
    scratch += scratches((s, width), dtype=F32) + scratches(*[(HALVES, T, whole)] * 3) + scratches((width, whole), (width, whole), (whole, width), (rows_in(ot), width), dtype=F32)
    scratch += [pltpu.SemaphoreType.DMA((HALVES * N, 3 * N))]
    for _ in range(quarters):
        scratch += scratches(*piece_shapes(packed, width)) + Ring.scratch(packed, width)
    if sent:
        scratch += Ring.scratch(*sent[FIRST].shape) + Ring.fetched(*sent[FIRST].shape)
    out = structs([(s, width), *sums]) + [struct((8, width), F32)] + structs(pieces)
    return pl.pallas_call(
        functools.partial(hidden_back, layer=layer, incoming=incoming, quarters=quarters, plan=plan),
        grid=(NEXT,),
        in_specs=[ANY] * (6 + len(sent) + plan[FIRST]),
        out_specs=[once(t.shape) for t in out] + [ANY] * len(plan[NEXT]),
        out_shape=out + plan[NEXT],
        scratch_shapes=scratch + Post.scratch(plan),
        compiler_params=talking(collective_id),
        cost_estimate=cost(16 * s * width * ff, 20),
    )(h1, dy, ot, wg, wu, wd, *sent, *letters)


def pass_attention_back(layer, x, low, high, weights, saved, dh1, sent, has_dx, letters, plan, collective_id, squares=(), count=FIRST):
    q, k, v, o, lse = saved
    s, width, d = rows_in(x), lanes(x), lanes(weights[FIRST])
    heads, blocks = d // HEAD, s // T
    down = lambda i: blocks - NEXT - i
    side, wide = heads * T, d + HALVES * HEAD
    pieces = piece_shapes(wide // N, width)
    out = structs([sent[FIRST].shape]) + [struct((8, width), F32)] + structs(pieces)
    specs = [once(t.shape) for t in out]
    more = []
    if has_dx:
        out, specs = [struct(x.shape)] + out, [states_spec(width, down)] + specs
    else:
        more = scratches(*pieces) + Ring.scratch(*pieces[FIRST]) + scratches((8, width), (N, 8, HEAD), dtype=F32) + [pltpu.SemaphoreType.DMA((N - NEXT,))] * HALVES
        out = structs([sent[FIRST].shape, pieces[FIRST]]) + [struct((8, width), F32)]
        specs = [once(t.shape) for t in out]
    return pl.pallas_call(
        functools.partial(attention_back, has_dx=has_dx, plan=plan, parts=len(squares), count=count),
        grid=(blocks,),
        in_specs=[states_spec(width, down), *angle_specs(down)] + [once(w.shape, layer) for w in weights]
        + [rows_spec(d, down), once(k.shape), once(v.shape), columns_spec(d, down), columns_spec(8, down), rows_spec(width, down)] + [ANY] * (len(sent) + plan[FIRST]) + [once(t.shape) for t in squares],
        out_specs=specs + [ANY] * len(plan[NEXT]),
        out_shape=out + plan[NEXT],
        scratch_shapes=scratches((width, wide), *[(HEAD, side)] * HALVES, *[(side, HALVES * HEAD)] * HALVES, *[(s, HALVES * HEAD)] * 3)
        + scratches((side, HALVES * HEAD), *[(HALVES * blocks, HEAD, HALF)] * HALVES, dtype=F32) + scratches((T, wide)) + scratches((width, wide), dtype=F32)
        + Ring.scratch(*sent[FIRST].shape) + Ring.fetched(*sent[FIRST].shape) + more + Post.scratch(plan),
        compiler_params=talking(collective_id),
        cost_estimate=cost(HALVES * s * d * (4 * s + 5 * width), 20),
    )(x, low, high, *weights, q, k, v, o, lse, dh1, *sent, *letters, *squares)


def packing(columns, rows, width):
    deep, at, table = width // N, FIRST, []
    for which, wide in enumerate(columns):
        start = FIRST
        while start < wide:
            take = min(wide - start, width - at % width)
            table.append((which, start, take, at // width * deep, at % width, deep, FIRST, deep))
            start, at = start + take, at + take
    return table + [(len(columns), FIRST, width, at // width * deep, FIRST, rows // N, FIRST, rows // N)]


def hidden_packing(width, ff, half):
    deep, slabs = width // N, ff // width // HALVES
    table = [(4 + m, (half * slabs + k) * width, width, (m * slabs + k) * deep, FIRST, deep, FIRST, deep) for m in range(HALVES) for k in range(slabs)]
    return table + down_packing(width, ff, half, HALVES * slabs * deep)


def down_packing(width, ff, half, row=FIRST):
    rows = ff // N
    return [(6, FIRST, width, row, FIRST, rows // HALVES, half * rows // HALVES, rows)]


def adamw(w, m, v, g):
    m = 0.9 * m + 0.1 * g
    v = 0.95 * v + 0.05 * g * g
    step = m * lax.rsqrt(v + 1e-8) + 0.1 * w
    return (w - 0.02 * step).astype(BF), m, v


def attention_step(me_ref, qkv_ref, rest_ref, factor_ref, *refs, table):
    (w, m, v), (new_m, new_v), out = (refs[i : i + 4] for i in range(FIRST, 12, 4)), (refs[-9:-5], refs[-5:-NEXT]), refs[-NEXT]
    for which, start, wide, row, lane, rows, *_ in table:
        here, there = slice(start, start + wide), (slice(row, row + rows), slice(lane, lane + wide))
        g_ref, at = (rest_ref, rows_in(rest_ref) - rows) if which == 3 else (qkv_ref, row)
        g = g_ref[at : at + rows, lane : lane + wide].astype(F32) * factor_ref[:NEXT, :wide]
        out[there], new_m[which][FIRST, :, here], new_v[which][FIRST, :, here] = adamw(
            w[which][FIRST, :, here].astype(F32), m[which][FIRST, :, here], v[which][FIRST, :, here], g)


def pass_attention_step(layer, me, gradients, factor, w, m, v, table, earlier):
    mine = [pl.BlockSpec((NEXT, *one.shape[NEXT:]), lambda i, me_ref: (layer, me_ref[FIRST], FIRST)) for one in m]
    moments = [pl.BlockSpec((NEXT, *one.shape[NEXT:]), lambda i, me_ref: (layer, FIRST, FIRST)) for one in m]
    packed = (table[-NEXT][3] + table[-NEXT][5], lanes(factor))
    return pl.pallas_call(
        functools.partial(attention_step, table=table),
        grid_spec=pltpu.PrefetchScalarGridSpec(
            num_scalar_prefetch=NEXT,
            grid=(NEXT,),
            in_specs=[once(t.shape) for t in (*gradients, factor)] + mine + moments * HALVES + [ANY] * len(earlier),
            out_specs=moments * HALVES + [once(packed)],
        ),
        out_shape=[struct(t.shape, F32) for t in m] * HALVES + structs([packed]),
        input_output_aliases={16 + k: k for k in range(len(earlier))},
        compiler_params=params(),
        cost_estimate=cost(HALVES**31, 8),
    )(me, *gradients, factor, *w, *m, *v, *earlier)


def hidden_step(me_ref, g0_ref, g1_ref, g_ref, factor_ref, *refs, layer):
    w, m, v, refs = refs[:3], refs[3:6], refs[6:9], refs[-10 if layer else -8 :]
    moments, outs = refs[:6], refs[6:]
    r = pl.program_id(FIRST)
    deep = rows_in(g0_ref) // 3
    quarters = [(g0_ref, FIRST), (g1_ref, FIRST), (g_ref, FIRST), (g_ref, 3 * deep)]

    def change(which, g):
        new, moments[which][FIRST], moments[which + 3][FIRST] = adamw(w[which][FIRST].astype(F32), m[which][FIRST], v[which][FIRST], g.astype(F32) * factor_ref[:NEXT])
        if layer and which < HALVES:
            outs[which][FIRST] = new
        for half in range(HALVES):

            @pl.when(lax.div(r, HALVES) == half)
            def _():
                if not layer:
                    outs[half][which] = new
                elif which == HALVES:
                    outs[HALVES + half][:] = new

    for which in range(HALVES):
        change(which, jnp.concatenate([ref[pl.ds(row + which * deep, deep), block(r, HEAD)] for ref, row in quarters], NEXT))
    for k, (ref, row) in enumerate(quarters):
        pl.when(r == k)(lambda ref=ref, row=row: change(HALVES, ref[pl.ds(row + HALVES * deep, deep), :]))


def pass_hidden_step(layer, me, gradients, factor, w, m, v, earlier):
    width = lanes(factor)
    rows = width // N
    slabs = width // rows
    tile = (NEXT, rows, width)
    wide, deep = pl.BlockSpec(tile, lambda c, _: (layer, FIRST, c)), pl.BlockSpec(tile, lambda c, _: (layer, c, FIRST))
    w_wide = pl.BlockSpec(tile, lambda c, me_ref: (layer, me_ref[FIRST], c))
    w_deep = pl.BlockSpec(tile, lambda c, me_ref: (layer, me_ref[FIRST] * slabs + c, FIRST))
    moments = [wide, wide, deep] * HALVES
    halves = [lambda c, _: jnp.minimum(c, NEXT), lambda c, _: jnp.maximum(c - HALVES, FIRST)]
    if layer:
        specs = [w_wide] * HALVES + [pl.BlockSpec((rows, width), lambda c, _, at=at: (at(c, _), FIRST)) for at in halves]
        shapes = structs([w[FIRST].shape] * HALVES + [(HALVES * rows, width)] * HALVES)
    else:
        specs = [pl.BlockSpec((3, rows, width), lambda c, _, at=at: (FIRST, at(c, _), FIRST)) for at in halves]
        shapes = structs([(3, HALVES * rows, width)] * HALVES)
    return pl.pallas_call(
        functools.partial(hidden_step, layer=layer),
        grid_spec=pltpu.PrefetchScalarGridSpec(
            num_scalar_prefetch=NEXT,
            grid=(slabs,),
            in_specs=[once(t.shape) for t in (*gradients, factor)] + [w_wide, w_wide, w_deep] + moments + [ANY] * len(earlier),
            out_specs=moments + specs,
        ),
        out_shape=[struct(t.shape, F32) for t in (*m, *v)] + shapes,
        input_output_aliases={14 + k: k for k in range(len(earlier))},
        compiler_params=params(),
        cost_estimate=cost(HALVES**32, 16),
    )(me, *gradients, factor, *w, *m, *v, *earlier)


def far_step(me_ref, factor_ref, *refs, pieces):
    gradients, refs = refs[:N], refs[N:]
    mine, others, w, outs = refs[:pieces], refs[pieces : HALVES * pieces], refs[HALVES * pieces : HALVES * pieces + HALVES], refs[-HALVES:]
    first = lax.rem(lax.axis_index("rep"), HALVES) == FIRST
    deep = rows_in(outs[FIRST])
    got = []
    for own in (mine, others):
        tiles = [t[:].reshape(-NEXT, lanes(outs[FIRST])) for t in own]
        got.append((tiles[FIRST], jnp.concatenate(tiles[NEXT:], FIRST)))
    for which, (w_ref, out) in enumerate(zip(w, outs)):
        a, b = got[FIRST][which], got[NEXT][which]
        g = jnp.concatenate([t[:].reshape(-NEXT, HEAD)[which * deep : (which + NEXT) * deep] for t in gradients], NEXT)
        out[FIRST] = adamw(w_ref[FIRST].astype(F32), jnp.where(first, a, b), jnp.where(first, b, a), g.astype(F32) * factor_ref[:NEXT])[FIRST]


def pass_far_step(step, me, factor, gradients, mine, others, at, w, outs):
    width = lanes(factor)
    rows = width // N

    def spec(shape, places):
        return pl.BlockSpec(shape, lambda c, _: (*places, FIRST, c))

    there = pl.BlockSpec((NEXT, rows, width), lambda c, me_ref: (NEXT, lax.rem(me_ref[FIRST] + step, N), c))
    tiles = [spec((*shape, rows // HALVES, width), places) for _, shape, places in at]
    return pl.pallas_call(
        functools.partial(far_step, pieces=len(at)),
        grid_spec=pltpu.PrefetchScalarGridSpec(
            num_scalar_prefetch=NEXT,
            grid=(lanes(outs[FIRST]) // width,),
            in_specs=[once(factor.shape)] + [spec((NEXT,) * len(places) + (HALVES * rows, HEAD), places) for _, places in gradients] + tiles * HALVES
            + [there] * HALVES + [ANY] * HALVES,
            out_specs=[there] * HALVES,
        ),
        out_shape=structs(t.shape for t in outs),
        input_output_aliases={HALVES + N + HALVES * len(at) + HALVES + k: k for k in range(HALVES)},
        compiler_params=params(),
        cost_estimate=cost(HALVES**31, 8),
    )(me, factor, *(g for g, _ in gradients), *(mine[k] for k, *_ in at), *(others[k] for k, *_ in at), *w, *outs)


def lay_out(me_ref, *refs, plan):
    count = len(plan)
    given, outs, held, (in_sem, out_sem) = refs[:count], refs[-count - 9 : -count - HALVES], refs[-count - HALVES : -HALVES], refs[-HALVES:]
    loads = [pltpu.make_async_copy(src, dst, in_sem.at[k]) for k, (src, dst) in enumerate(zip(given, held))]
    for copy in loads:
        copy.start()
    stores = []
    for k, (step, layer, table) in enumerate(plan):
        owner = lax.rem(me_ref[FIRST] + step, N)
        loads[k].wait()
        for which, start, wide, row, lane, rows, base, deep in table:
            to = outs[which].at[layer, pl.ds(pl.multiple_of(owner * deep + base, 32), rows), pl.ds(start, wide)]
            stores.append(pltpu.make_async_copy(held[k].at[pl.ds(row, rows), pl.ds(lane, wide)], to, out_sem.at[len(stores)]))
            stores[-NEXT].start()
    for copy in stores:
        copy.wait()


def pass_lay_out(me, blocks, plan, shapes, earlier):
    stores = sum(len(table) for *_, table in plan)
    return pl.pallas_call(
        functools.partial(lay_out, plan=plan),
        grid_spec=pltpu.PrefetchScalarGridSpec(
            num_scalar_prefetch=NEXT,
            grid=(NEXT,),
            in_specs=[ANY] * (len(blocks) + len(earlier)),
            out_specs=[ANY] * len(shapes),
            scratch_shapes=scratches(*(t.shape for t in blocks)) + [pltpu.SemaphoreType.DMA((len(blocks),)), pltpu.SemaphoreType.DMA((stores,))],
        ),
        out_shape=structs(shapes),
        input_output_aliases={NEXT + len(blocks) + k: which for k, which in enumerate(earlier)},
        compiler_params=params(),
        cost_estimate=cost(HALVES**31, 16),
    )(me, *blocks, *earlier.values())


def plans(rows, wide, packed, width, last):
    half = rows // HALVES
    top, low = pl.ds(FIRST, half), pl.ds(half, half)
    both = ("right", "left")
    moments = lambda *lead: struct((*lead, half, wide), F32)
    sums = lambda *lead: struct((*lead, HALVES * rows, width))
    used = pl.ds(FIRST, HALVES * rows)

    def first(letters, arrived):
        m_gate, m_up, v_gate, v_up = (ref.at[last] for ref in letters)
        pairs = ((m_gate.at[top], v_gate.at[top]), (m_gate.at[low], v_gate.at[low]), (m_up.at[top], v_up.at[top]))
        return [(pair, arrived[FIRST].at[k, n], way) for n, pair in enumerate(pairs) for k, way in enumerate(both)]

    def second(letters, arrived):
        m_up, v_up, t1 = letters
        t2, x1 = arrived
        pair = (m_up.at[last, low], v_up.at[last, low])
        return [(pair, t2.at[k], way) for k, way in enumerate(both)] + [
            (t1.at[FIRST, FIRST], t2.at[HALVES], "right"), (t1.at[NEXT, NEXT], t2.at[3], "left"), (t1, x1, "other")]

    def third(letters, arrived):
        (t1, t2), (t3, x2) = letters, arrived
        return [(t1.at[FIRST, HALVES], t3.at[FIRST], "right"), (t2.at[NEXT], t3.at[NEXT], "left"), (t2, x2, "other")]

    def fourth(letters, arrived):
        t3, *quarters = letters
        x3, y1 = arrived
        return [(q.at[used], y1.at[k, n], way) for n, q in enumerate(quarters) for k, way in enumerate(both)] + [(t3, x3, "other")]

    def fifth(letters, arrived):
        return [(letters[FIRST].at[pl.ds(n * packed, HALVES * rows)], arrived[FIRST].at[k, n], way) for n in range(HALVES) for k, way in enumerate(both)]

    def sixth(letters, arrived):
        return [(come.at[k, k], on.at[k], way) for come, on in zip(letters, arrived) for k, way in enumerate(both)]

    return ((4, [moments(HALVES, 3)], first, 6), (3, [moments(4), moments(HALVES, 3)], second, 5), (HALVES, [moments(HALVES), moments(4)], third, 3),
            (3, [moments(HALVES), sums(HALVES, HALVES)], fourth, 5), (NEXT, [sums(HALVES, HALVES)], fifth, 4), (HALVES, [sums(HALVES), sums(HALVES)], sixth, 4))


def solution(mesh):
    n = mesh.shape["dp"]

    def step(x, dy, *arrays):
        weights, m, v = (arrays[i : i + 7] for i in (FIRST, 7, 14))
        me = lax.axis_index("dp")[None].astype(jnp.int32)
        width, d, ff, layers = rows_in(weights[FIRST]), lanes(weights[FIRST]), lanes(weights[4]), weights[FIRST].shape[FIRST]
        low_high = tables(rows_in(x))
        attn, hidden = weights[:4], weights[4:]
        (m_gate, m_up), (v_gate, v_up) = m[4:6], v[4:6]
        plan = plans(rows_in(m_gate), ff, 3 * width // N, width, layers - NEXT)
        *saved0, h1, h, t1 = pass_forward(FIRST, x, *low_high, weights, [m_gate, m_up, v_gate, v_up], plan[FIRST], NEXT)
        *saved1, h1_last, t2, x1 = pass_forward(NEXT, h, *low_high, attn, [m_up, v_up, t1], plan[NEXT], HALVES)
        dh1, q0, q1, squares0, *sent, t3, x2 = pass_hidden_back(NEXT, h1_last, dy, saved1[3], *hidden, [], [t1, t2], plan[HALVES], 3)
        dh, rest, squares1, *sent, x3, y1 = pass_attention_back(NEXT, h, *low_high, attn, saved1, dh1, sent, True, [t3, q0, q1], plan[3], 4)
        g_hidden1 = q0, q1, rest
        dh1, q0, q1, g_qkv1, squares2, *sent, y2 = pass_hidden_back(FIRST, h1, dh, saved0[3], *hidden, sent, [rest], plan[4], 5)
        squares, count = [squares0, squares1, squares2], n * sum(one.size for one in m)
        rest, g_qkv0, factor, y3, y4 = pass_attention_back(FIRST, x, *low_high, attn, saved0, dh1, sent, False, [y1, y2], plan[5], 6, squares, count)
        g_hidden0 = q0, q1, rest

        ways = {"right": [(i, (i + NEXT) % n) for i in range(n)], "left": [(i, (i - NEXT) % n) for i in range(n)]}

        def send(way, t):
            return lax.ppermute(t, "dp", ways[way])

        table = packing((d, HEAD, HEAD), d, width)
        tables_ = {"a0": (FIRST, table), "a1": (NEXT, table)}
        for half, name in enumerate("xy"):
            tables_["h" + name] = (FIRST, hidden_packing(width, ff, half))
            tables_["d" + name] = (NEXT, down_packing(width, ff, half))
        *moments_a, a0 = pass_attention_step(FIRST, me, (g_qkv0, g_hidden0[HALVES]), factor, attn, m[:4], v[:4], table, ())
        *moments_a, a1 = pass_attention_step(NEXT, me, (g_qkv1, g_hidden1[HALVES]), factor, attn, m[:4], v[:4], table, moments_a)
        *moments_h, hx, hy = pass_hidden_step(FIRST, me, g_hidden0, factor, hidden, m[4:], v[4:], ())
        *moments_h, gate, up, dx, dy_ = pass_hidden_step(NEXT, me, g_hidden1, factor, hidden, m[4:], v[4:], moments_h)
        mine, others = (t1, t2, t3), (x1, x2, x3)
        for step_, side in ((3, FIRST), (NEXT, NEXT)):
            at = ((FIRST, (NEXT, HALVES), (side, FIRST)), (FIRST, (NEXT, NEXT), (side, HALVES)), (NEXT, (NEXT,), (side,)))
            gate, up = pass_far_step(step_, me, factor, [(y, (side, k)) for y in (y1, y2) for k in range(HALVES)], mine, others, at, hidden[:HALVES], (gate, up))
        at = ((NEXT, (HALVES,), (NEXT,)), (HALVES, (HALVES,), (FIRST,)))
        gate, up = pass_far_step(HALVES, me, factor, [(y, (k,)) for y in (y3, y4) for k in range(HALVES)], mine, others, at, hidden[:HALVES], (gate, up))
        own = {"a0": a0, "a1": a1, "hx": hx.reshape(-NEXT, width), "hy": hy.reshape(-NEXT, width), "dx": dx, "dy": dy_}
        came = {way: {name: send(way, t) for name, t in own.items()} for way in ways}
        on = {name: "right" if name[NEXT] in "0x" else "left" for name in own}
        across = [send(way, came[way][name]) for name, way in on.items()]
        shapes = [w.shape for w in weights]
        blocks, where = [], []
        for step_, given in ((FIRST, own), (n - NEXT, came["right"]), (NEXT, came["left"])):
            blocks += given.values()
            where += [(step_, *tables_[name]) for name in given]
        new = pass_lay_out(me, blocks, where, shapes, {4: gate, 5: up})
        for part in (slice(FIRST, 4), slice(4, 6)):
            new = pass_lay_out(me, across[part], [(HALVES, *tables_[name]) for name in [*on][part]], shapes, dict(enumerate(new)))
        return (*new, *moments_a[:4], *moments_h[:3], *moments_a[4:], *moments_h[3:])

    states, all_of, cut = P(("rep", "dp"), None, None), P(None, None, None), P(None, "dp", None)
    return jax.shard_map(
        step,
        mesh=mesh,
        in_specs=(states, states) + (all_of,) * 7 + (cut,) * 14,
        out_specs=(P("rep", None, None),) * 7 + (P("rep", "dp", None),) * 14,
        check_vma=False,
    )
```
